256 devices in a mesh: freq: 8 (over y, x_hi), rec: 32 (over x_lo, z, core).
Axes of the slice: x: 4 (x_hi: 2, x_lo: 2; x = x_hi * 2 + x_lo), y: 4, z: 8, core: 2. Of those that a mesh axis runs over, the one named last changes fastest.
Arguments:
- response: bfloat16 [128, 2, 1792, 1792], P('freq', None, 'rec'), may hold values from -1 to 1, as said below
- direct: float32 [1792, 32, 256], P('rec', 'freq'), may hold values from -6 to 6
- onset: int32 [1792, 32], P('rec', 'freq'), may hold values from 16 to 128
Outputs:
- upgoing: float32 [1792, 32, 256], P('rec', 'freq')
- coda: float32 [1792, 32, 256], P('rec', 'freq')
The draws below stay inside these ranges and needn't reach their ends.
Inputs may be any that keep to these rules, and one draw needn't show every extreme that they name: response[k, c, r, s] = response[k, c, s, r] for every frequency and part (source-receiver reciprocity).
All inputs are finite; a program needn't handle non-finite values.
Results may differ from the reference program's by a relative error of at most 0.023.
Values may be sent and summed in bfloat16 or wider, within the bound.
A program may use at most 128 MiB of HBM per device.

```python
import math
import jax
import jax.numpy as jnp
from jax import lax

NS = 1792
NF = 128
NT = 256
NV = 32
ITERS = 2


def draw_response(key, part):
    subkeys = jax.random.split(jax.random.fold_in(key, 17), NF)

    def per_frequency(subkey):
        entries = jnp.clip(jax.random.normal(subkey, (2, NS, NS), jnp.float32), -4.0, 4.0)
        paired = (entries + jnp.swapaxes(entries, 1, 2)) * 0.5 ** 0.5
        return (paired * (2.0 * NS) ** (-0.5)).astype(jnp.bfloat16)
    return lax.map(per_frequency, subkeys)


def plant(result, own_key, smallest, top_value):
    extent = result.shape
    spot = [jax.random.randint(jax.random.fold_in(own_key, axis), (), 0, extent[axis]) for axis in range(len(extent))]
    result = result.at[tuple(spot)].set(smallest)
    longest = extent.index(max(extent))
    spot[longest] = (spot[longest] + 1) % extent[longest]
    return result.at[tuple(spot)].set(top_value)


def level_of(own_key, extent, pieces, smallest, high):
    factor_of, own = 1.0, jax.random.fold_in(own_key, 6)
    for position, blocks in pieces:
        draws = jnp.exp(jax.random.uniform(jax.random.fold_in(own, position), (blocks,), jnp.float32, smallest / len(pieces), high / len(pieces)))
        factor_of = factor_of * jnp.repeat(draws, extent[position] // blocks).reshape([-1 if axis == position else 1 for axis in range(len(extent))])
    return factor_of


def normal_values(rng, extent, scale, most, cuts=(), held_as=jnp.bfloat16):
    drawn = scale * jax.random.normal(rng, extent, jnp.float32)
    if cuts:
        drawn = drawn * level_of(rng, extent, cuts, -0.22, 0.18)
    return jnp.clip(drawn, -most, most).astype(held_as)


def setup_inputs(seed: int = 0) -> dict:
    key_list = jax.random.split(jax.random.key(seed), 4)
    response = draw_response(jax.random.fold_in(key_list[3], 71), 0)
    direct = normal_values(key_list[1], (NS, NV, NT), 1.0, 6.0, ((0, 32), (1, 8)), jnp.float32)
    onset = plant(jax.random.randint(key_list[2], (NS, NV), NT // 16, NT // 2 + 1), jax.random.fold_in(key_list[2], 1), NT // 16, (NT // 2 + 1) - 1).astype(jnp.int32)
    return {"response": response, "direct": direct, "onset": onset}


def spectral_tables(length, count):
    samples = jnp.arange(length, dtype=jnp.int32)
    frequency_bins = jnp.arange(1, count + 1, dtype=jnp.int32)
    phase = ((samples[:, None] * frequency_bins[None, :]) % length).astype(jnp.float32) * (2.0 * math.pi / length)
    cosine = jnp.cos(phase)
    sine = jnp.sin(phase)
    forward = jnp.concatenate([cosine, -sine], axis=1)
    inverse = jnp.concatenate([cosine.T, -sine.T], axis=0) * (2.0 / length)
    return forward, inverse


def make_window(onset, length):
    samples = jnp.arange(length, dtype=jnp.int32)
    folded = jnp.minimum(samples, length - samples)
    return (folded[None, None, :] < onset[:, :, None]).astype(jnp.float32)


def to_spectrum(field, forward):
    packed = jnp.dot(field, forward, precision=lax.Precision.HIGHEST).astype(jnp.bfloat16)
    return packed.reshape(field.shape[0], field.shape[1], 2, forward.shape[1] // 2)


def to_time(spectra, inverse):
    flat = spectra.reshape(spectra.shape[0], spectra.shape[1], -1).astype(jnp.float32)
    return jnp.dot(flat, inverse, precision=lax.Precision.HIGHEST)


def convolve(response, spectra, adjoint):
    moved = jnp.transpose(spectra, (3, 0, 1, 2))

    def per_frequency(unused_state, frequency_slice):
        matrix, vectors = frequency_slice
        real_matrix = matrix[0]
        imag_matrix = matrix[1]
        if adjoint:
            real_matrix = real_matrix.T
            imag_matrix = -imag_matrix.T
        vec_real = vectors[:, :, 0]
        vec_imag = vectors[:, :, 1]
        out_real = jnp.dot(real_matrix, vec_real, preferred_element_type=jnp.float32) - jnp.dot(imag_matrix, vec_imag, preferred_element_type=jnp.float32)
        out_imag = jnp.dot(real_matrix, vec_imag, preferred_element_type=jnp.float32) + jnp.dot(imag_matrix, vec_real, preferred_element_type=jnp.float32)
        return unused_state, jnp.stack([out_real, out_imag], axis=2)

    unused_final, stacked = lax.scan(per_frequency, jnp.zeros((), jnp.float32), (response, moved))
    return jnp.transpose(stacked, (1, 2, 3, 0)).astype(jnp.bfloat16)


def reference(response, direct, onset):
    forward, inverse = spectral_tables(NT, NF)
    window = make_window(onset, NT)
    coda = jnp.zeros_like(direct)
    upgoing = coda
    for iteration in range(ITERS):
        downgoing = direct + coda
        spectra = to_spectrum(downgoing, forward)
        reflected = convolve(response, spectra, False)
        upgoing = window * to_time(reflected, inverse)
        spectra_up = to_spectrum(upgoing, forward)
        returned = convolve(response, spectra_up, True)
        coda = window * to_time(returned, inverse)
    return upgoing, coda
```

```python
import math

import jax
import jax.numpy as jnp
import numpy as np
from jax import lax
from jax.experimental import pallas as pl
from jax.experimental.pallas import tpu as pltpu
from jax.sharding import PartitionSpec as P

NF, NT, ITERS = 128, 256, 2
NS, ROWS, NVD, NFD = 1792, 56, 4, 8
NZ = 8
CHUNKS = 1
V = NVD // CHUNKS
G = 8 // V
LC = 64 * V
MESH = pl.DeviceIdType.MESH
F32, BF16 = jnp.float32, jnp.bfloat16
ZS, XS = pl.ds(0, V // 2), pl.ds(V // 2, V // 2)


def tables():
    rho = np.arange(256)
    kg = rho % G
    part = (rho // G) % 2
    kp = (rho // (2 * G)) % V
    band = rho // 16
    bins = band * 8 + kp * G + kg + 1
    phase = ((np.arange(NT)[None, :] * bins[:, None]) % NT).astype(np.float64) * (2.0 * math.pi / NT)
    table = np.where(part[:, None] == 0, np.cos(phase), -np.sin(phase)).astype(np.float32)
    return jnp.asarray(table, dtype=BF16), jnp.asarray((table * (2.0 / NT)).T, dtype=BF16)


def lane_bit(shape, stride):
    lanes = lax.broadcasted_iota(jnp.int32, shape, len(shape) - 1)
    return (lanes // stride) % 2 == 0


def exchange(arrays):
    shape = arrays[0].shape
    stride, span = 2 * G, 1
    while span < V:
        low = lane_bit(shape, stride)
        out = list(arrays)
        for i in range(V):
            if (i // span) % 2 == 0:
                first, second = arrays[i], arrays[i + span]
                out[i] = jnp.where(low, first, pltpu.roll(second, stride, 1))
                out[i + span] = jnp.where(low, pltpu.roll(first, 128 - stride, 1), second)
        arrays = out
        stride, span = stride * 2, span * 2
    return arrays


def kernel(
    resp, direct, onset, fwd, inv, up_out, coda_out,
    rs, x, sf, rf, sb, rb, dt, fb, prod,
    r_sem, af_s, af_r, ab_s, ab_r, z_s, z_r, x_s, x_r,
):
    f = lax.axis_index("freq")
    p = lax.axis_index("rec")
    a, z, q = p // 16, (p // 2) % NZ, p % 2

    def dev(df=0, dz=0, dq=0, da=0):
        return ((f + df) % NFD, ((a + da) % 2) * 16 + ((z + dz + NZ) % NZ) * 2 + (q + dq) % 2)

    def row(a_, z_):
        return pl.multiple_of((a_ * NZ + z_) * 112, 16)

    peers = [dev(dz=1), dev(dz=-1), dev(da=1)]
    freq_peers = [(df, dq) for df in range(NFD) for dq in range(2) if df or dq]

    own_r = pltpu.make_async_copy(resp.at[pl.ds(q * 8, 8)], rs.at[:, q], r_sem.at[0])
    own_r.start()

    barrier = pltpu.get_barrier_semaphore()
    for peer in peers + [dev(df=df, dq=dq) for df, dq in freq_peers]:
        pl.semaphore_signal(barrier, inc=1, device_id=peer, device_id_type=MESH)
    pl.semaphore_wait(barrier, len(peers) + len(freq_peers))

    other_r = pltpu.make_async_remote_copy(
        src_ref=resp.at[pl.ds((1 - q) * 8, 8)], dst_ref=rs.at[:, q],
        send_sem=r_sem.at[1], recv_sem=r_sem.at[2], device_id=dev(dq=1), device_id_type=MESH)
    other_r.start()

    def spread(src_slot, dst, dst_slot, sends, recvs, ch):
        return [
            pltpu.make_async_remote_copy(
                src_ref=src_slot((f + df) % NFD, (q + dq) % 2), dst_ref=dst_slot(dst),
                send_sem=sends.at[ch, 2 * df + dq], recv_sem=recvs.at[ch, 2 * df + dq],
                device_id=dev(df=df, dq=dq), device_id_type=MESH)
            for df, dq in freq_peers]

    def sf_slot(ch):
        return lambda fd, qd: sf.at[ch, pl.ds(pl.multiple_of((fd * 2 + qd) * 16, 16), 16)]

    def sb_slot(ch):
        return lambda fd, qd: sb.at[ch, qd, pl.ds(pl.multiple_of(fd * 16, 16), 16)]

    def forward_copies(ch):
        return spread(sf_slot(ch), rf, lambda d: d.at[ch, q, pl.ds(pl.multiple_of(f * 16, 16), 16)], af_s, af_r, ch)

    def back_copies(ch):
        return spread(sb_slot(ch), rb, lambda d: d.at[ch, pl.ds(pl.multiple_of((f * 2 + q) * 16, 16), 16)],
                      ab_s, ab_r, ch)

    def analyse(ch, field):
        sf[ch] = jnp.dot(fwd[...], field.astype(BF16), preferred_element_type=F32).astype(BF16)
        for copy in forward_copies(ch):
            copy.start()
        rf[ch, q, pl.ds(pl.multiple_of(f * 16, 16), 16)] = sf[ch, pl.ds(pl.multiple_of((f * 2 + q) * 16, 16), 16)]

    def collect(ch, par):
        for copy in forward_copies(ch):
            copy.wait_recv()
        for copy in forward_copies(ch):
            copy.wait_send()
        halves = []
        for core in range(2):
            parts = []
            for pair in range(V // 2):
                block = rf[ch, core, :, pair * 128:(pair + 1) * 128].astype(F32).T
                parts += [block[0:ROWS], block[ROWS:2 * ROWS]]
            halves.append(exchange(parts))
        for kp in range(V):
            x[par, ch, kp, pl.ds(row(a, z), 112), :] = jnp.concatenate(
                [halves[0][kp], halves[1][kp]], axis=0).astype(BF16)

    def last_hop(ch, way, unit):
        far = (0, 1, ch % 2)[unit]
        return 4 if way == far else 3

    def z_copy(ch, par, way, hop, unit):
        step = 1 if way == 0 else -1
        source_z = (z - step * (hop - 1) + NZ) % NZ
        ref = x.at[par, ch, XS if unit == 2 else ZS, pl.ds(row((a + 1) % 2 if unit == 1 else a, source_z), 112)]
        return pltpu.make_async_remote_copy(
            src_ref=ref, dst_ref=ref, send_sem=z_s.at[ch, way, hop - 1, unit],
            recv_sem=z_r.at[par, ch, way, hop - 1, unit], device_id=dev(dz=step), device_id_type=MESH)

    def z_arrival(ch, par, way, hop, unit):
        step = 1 if way == 0 else -1
        source_z = (z - step * hop + NZ) % NZ
        ref = x.at[par, ch, XS if unit == 2 else ZS, pl.ds(row((a + 1) % 2 if unit == 1 else a, source_z), 112)]
        return pltpu.make_async_remote_copy(
            src_ref=ref, dst_ref=ref, send_sem=z_s.at[ch, way, hop - 1, unit],
            recv_sem=z_r.at[par, ch, way, hop - 1, unit], device_id=dev(dz=step), device_id_type=MESH)

    def x_copy(ch, par, slot, mine):
        source_z = z if slot == 8 else (z - slot + NZ) % NZ
        ref = x.at[par, ch, ZS if slot == 8 else XS, pl.ds(row(a if mine else (a + 1) % 2, source_z), 112)]
        return pltpu.make_async_remote_copy(
            src_ref=ref, dst_ref=ref, send_sem=x_s.at[ch, slot], recv_sem=x_r.at[par, ch, slot],
            device_id=dev(da=1), device_id_type=MESH)

    def ring_start(ch, par):
        x_copy(ch, par, 8, True).start()
        for unit in (0, 2):
            for way in range(2):
                z_copy(ch, par, way, 1, unit).start()
        x_copy(ch, par, 0, True).start()
        x_copy(ch, par, 8, False).wait_recv()
        for way in range(2):
            z_copy(ch, par, way, 1, 1).start()

    def ring_hop(ch, par, hop):
        for unit in (0, 2, 1):
            for way in range(2):
                if hop > last_hop(ch, way, unit):
                    continue
                z_arrival(ch, par, way, hop, unit).wait_recv()
                if hop < last_hop(ch, way, unit):
                    z_copy(ch, par, way, hop + 1, unit).start()
                if unit == 2:
                    x_copy(ch, par, hop if way == 0 else 8 - hop, True).start()

    def ring_end(ch, par):
        for slot in range(8):
            x_copy(ch, par, slot, False).wait_recv()

    def ring_drain(ch, par):
        for slot in range(9):
            x_copy(ch, par, slot, True).wait_send()
        for unit in range(3):
            for way in range(2):
                for hop in range(1, last_hop(ch, way, unit) + 1):
                    z_copy(ch, par, way, hop, unit).wait_send()

    def apply(ch, par, n):
        sign = jnp.where(n % 2 == 0, 1.0, -1.0).astype(F32)
        shape = (ROWS, 128)
        low = lane_bit(shape, G)
        lanes = lax.broadcasted_iota(jnp.int32, shape, 1)
        groups = [[], []]
        for kp in range(V):
            prod[...] = jnp.dot(
                rs[kp * G:(kp + 1) * G].reshape(G * 224, NS), x[par, ch, kp], preferred_element_type=F32)
            for core in range(2):
                re = im = None
                for kg in range(G):
                    base = kg * 224 + core * 112
                    re_k, im_k = prod[base:base + ROWS, :], prod[base + ROWS:base + 2 * ROWS, :]
                    mine = lanes % G == kg
                    re = re_k if re is None else jnp.where(mine, re_k, re)
                    im = im_k if im is None else jnp.where(mine, im_k, im)
                turned = jnp.where(low, -pltpu.roll(im, 128 - G, 1), pltpu.roll(im, G, 1))
                groups[core].append(re + sign * turned)
        for core in range(2):
            parts = exchange(groups[core])
            for pair in range(V // 2):
                block = jnp.concatenate(
                    [parts[2 * pair], parts[2 * pair + 1], jnp.zeros((16, 128), F32)], axis=0)
                sb[ch, core, :, pair * 128:(pair + 1) * 128] = block.T.astype(BF16)
        for copy in back_copies(ch):
            copy.start()
        rb[ch, pl.ds(pl.multiple_of((f * 2 + q) * 16, 16), 16)] = sb[ch, q, pl.ds(pl.multiple_of(f * 16, 16), 16)]

    def synthesise(ch, n):
        for copy in back_copies(ch):
            copy.wait_recv()
        for copy in back_copies(ch):
            copy.wait_send()
        t = lax.broadcasted_iota(jnp.int32, (NT, LC), 0)
        inside = jnp.minimum(t, NT - t) < onset[:, ch * LC:(ch + 1) * LC]
        field = jnp.where(inside, jnp.dot(inv[...], rb[ch], preferred_element_type=F32), 0.0)
        fb[n % 2, ch] = field
        return field

    for ch in range(CHUNKS):
        for pair in range(V // 2):
            first = ch * V + 2 * pair
            block = jnp.concatenate(
                [direct[:, first * NT:(first + 1) * NT], direct[:, (first + 1) * NT:(first + 2) * NT],
                 jnp.zeros((16, NT), F32)], axis=0)
            dt[ch, :, pair * 128:(pair + 1) * 128] = block.T
        analyse(ch, dt[ch])
    own_r.wait()
    other_r.wait()

    def step(n, carry):
        par = n % 2
        for ch in range(CHUNKS):
            collect(ch, par)
            ring_start(ch, par)
            for hop in range(1, 5):
                ring_hop(ch, par, hop)
            ring_end(ch, par)
            apply(ch, par, n)
            ring_drain(ch, par)
            field = synthesise(ch, n)

            @pl.when(n < 2 * ITERS - 1)
            def _():
                analyse(ch, jnp.where(n % 2 == 0, field, field + dt[ch]))
        return carry

    lax.fori_loop(0, 2 * ITERS, step, 0)

    for part, out in ((0, up_out), (1, coda_out)):
        for ch in range(CHUNKS):
            for pair in range(V // 2):
                block = fb[part, ch, :, pair * 128:(pair + 1) * 128].T
                for half in range(2):
                    v = ch * V + 2 * pair + half
                    out[:, v * NT:(v + 1) * NT] = block[half * ROWS:(half + 1) * ROWS]


def body(response, direct, onset):
    fwd, inv = tables()
    vmem = pl.BlockSpec(memory_space=pltpu.VMEM)
    lanes = jnp.pad(onset.T.reshape(2, 2 * ROWS), ((0, 0), (0, 16))).reshape(1, 256)
    dma = pltpu.SemaphoreType.DMA
    up, coda = pl.pallas_call(
        kernel,
        name="marchenko",
        out_shape=[jax.ShapeDtypeStruct((ROWS, NVD * NT), F32)] * 2,
        in_specs=[pl.BlockSpec(memory_space=pl.ANY), vmem, vmem, vmem, vmem],
        out_specs=[vmem, vmem],
        scratch_shapes=[
            pltpu.VMEM((8, 2, 112, NS), BF16),
            pltpu.VMEM((2, CHUNKS, V, NS, 128), BF16),
            pltpu.VMEM((CHUNKS, 256, LC), BF16),
            pltpu.VMEM((CHUNKS, 2, 128, LC), BF16),
            pltpu.VMEM((CHUNKS, 2, 128, LC), BF16),
            pltpu.VMEM((CHUNKS, 256, LC), BF16),
            pltpu.VMEM((CHUNKS, NT, LC), F32),
            pltpu.VMEM((2, CHUNKS, NT, LC), F32),
            pltpu.VMEM((G * 224, 128), F32),
            dma((3,)),
            dma((CHUNKS, 16)), dma((CHUNKS, 16)), dma((CHUNKS, 16)), dma((CHUNKS, 16)),
            dma((CHUNKS, 2, 4, 3)), dma((2, CHUNKS, 2, 4, 3)),
            dma((CHUNKS, 9)), dma((2, CHUNKS, 9)),
        ],
        compiler_params=pltpu.CompilerParams(
            collective_id=0, has_side_effects=True, vmem_limit_bytes=60 * 2**20),
    )(response.reshape(16, 112, NS), direct.reshape(ROWS, NVD * NT), lanes, fwd, inv)
    return up.reshape(ROWS, NVD, NT), coda.reshape(ROWS, NVD, NT)


def solution(mesh):
    placed = (P("freq", None, "rec", None), P("rec", "freq", None), P("rec", "freq"))
    return jax.shard_map(
        body, mesh=mesh, in_specs=placed,
        out_specs=(P("rec", "freq", None), P("rec", "freq", None)), check_vma=False)
```

```python
import math

import jax
import jax.numpy as jnp
import numpy as np
from jax import lax
from jax.experimental import pallas as pl
from jax.experimental.pallas import tpu as pltpu
from jax.sharding import PartitionSpec as P

NF, NT, ITERS = 128, 256, 2
NS, ROWS, NVD, NFD = 1792, 56, 4, 8
NZ = 8
CHUNKS = 1
V = NVD // CHUNKS
G = 8 // V
LC = 64 * V
MESH = pl.DeviceIdType.MESH
F32, BF16 = jnp.float32, jnp.bfloat16
SENDS = [
    (1, 0, 0, -1, 0), (3, 0, 0, -1, 0), (0, 0, 0, 1, 0), (0, 0, 0, 0, 1), (0, 0, 0, -2, 0), (2, 0, 0, 1, 0),
    (2, 0, 0, 0, 1), (3, 0, 0, 0, 1), (1, 0, 0, 0, 1), (3, 0, 0, 1, 0), (1, 0, 0, 2, 0), (2, 0, 0, -2, 0),
    (1, 0, 0, 1, 0), (0, 1, 0, 2, 0), (0, 1, 0, 1, 1), (1, -1, 0, -2, 0), (1, -1, 0, -1, 1), (2, 0, 1, -1, 1),
    (2, 1, 0, 2, 0), (2, 1, 0, 1, 1), (3, -1, 0, -3, 0), (3, -1, 0, -1, 1), (3, 0, 1, 1, 1), (3, 1, 0, 2, 0),
    (0, -2, 0, 4, 0), (0, -2, 0, -1, 0), (0, -2, 0, -2, 1), (1, 2, 0, 2, 1), (1, 2, 0, 3, 0), (2, -2, 0, -2, 1),
    (2, -2, 0, -3, 0), (0, 2, 0, 3, 0), (0, 2, 0, 2, 1), (1, -2, 0, -3, 0), (1, -1, 1, -2, 1), (2, 2, 0, 4, 0),
    (2, 2, 0, 2, 1), (2, -1, 1, -1, 0), (3, -1, 1, -2, 1), (3, 1, 1, 2, 1), (3, -3, 0, 4, 0), (3, -3, 0, -2, 0),
    (3, -3, 0, -3, 1), (0, -2, 1, -3, 1), (0, -1, 0, -1, 1), (1, 2, 1, 4, 1), (1, 2, 1, 1, 1), (1, 2, 1, 3, 1),
    (0, 3, 0, 3, 1), (0, 4, 0, -3, 0), (0, 4, 0, 4, 1), (2, -2, 1, -3, 1), (1, -3, 0, 4, 0), (1, -3, 0, -3, 1),
    (2, 2, 1, 3, 1), (3, 2, 1, 3, 1), (2, 4, 0, 3, 0), (2, 4, 0, 4, 1), (3, 4, 0, 3, 0), (3, 4, 0, 4, 1),
]
ARRIVALS = [
    (0, 0, 1), (0, 1, 0), (1, -1, 0), (2, 0, 1), (2, 1, 0), (3, -1, 0), (3, 0, 1), (3, 1, 0),
    (1, 0, 1), (0, -2, 0), (1, 1, 0), (1, 2, 0), (2, -2, 0), (0, 2, 0), (1, -2, 0), (1, -1, 1),
    (0, 1, 1), (2, 2, 0), (2, -1, 1), (3, -1, 1), (3, 1, 1), (2, 1, 1), (3, -3, 0), (3, 2, 0),
    (0, -2, 1), (0, -1, 0), (1, 2, 1), (1, 3, 0), (2, -3, 0), (0, 3, 0), (0, 4, 0), (2, -2, 1),
    (0, 2, 1), (1, -3, 0), (1, -2, 1), (2, 2, 1), (3, 2, 1), (2, -1, 0), (2, 4, 0), (3, -2, 1),
    (3, -3, 1), (3, -2, 0), (3, 4, 0), (0, -3, 1), (0, -1, 1), (0, 4, 1), (1, 1, 1), (1, 3, 1),
    (0, -3, 0), (0, 3, 1), (2, -3, 1), (1, -3, 1), (1, 4, 0), (1, 4, 1), (2, 3, 0), (2, 3, 1),
    (2, 4, 1), (3, 3, 0), (3, 3, 1), (3, 4, 1),
]


def tables():
    rho = np.arange(256)
    kg = rho % G
    part = (rho // G) % 2
    kp = (rho // (2 * G)) % V
    band = rho // 16
    bins = band * 8 + kp * G + kg + 1
    phase = ((np.arange(NT)[None, :] * bins[:, None]) % NT).astype(np.float64) * (2.0 * math.pi / NT)
    table = np.where(part[:, None] == 0, np.cos(phase), -np.sin(phase)).astype(np.float32)
    return jnp.asarray(table, dtype=BF16), jnp.asarray((table * (2.0 / NT)).T, dtype=BF16)


def scoped(function):
    def wrapped(*args):
        with jax.named_scope(function.__name__):
            return function(*args)
    return wrapped


def lane_bit(shape, stride):
    lanes = lax.broadcasted_iota(jnp.int32, shape, len(shape) - 1)
    return (lanes // stride) % 2 == 0


def exchange(arrays):
    shape = arrays[0].shape
    stride, span = 2 * G, 1
    while span < V:
        low = lane_bit(shape, stride)
        out = list(arrays)
        for i in range(V):
            if (i // span) % 2 == 0:
                first, second = arrays[i], arrays[i + span]
                out[i] = jnp.where(low, first, pltpu.roll(second, stride, 1))
                out[i + span] = jnp.where(low, pltpu.roll(first, 128 - stride, 1), second)
        arrays = out
        stride, span = stride * 2, span * 2
    return arrays


def kernel(
    resp, direct, onset, fwd, inv, up_out, coda_out,
    rs, x, sf, rf, sb, rb, dt, fb, prod, limits,
    r_sem, af_s, af_r, ab_s, ab_r, m_s, m_r,
):
    f = lax.axis_index("freq")
    p = lax.axis_index("rec")
    a, z, q = p // 16, (p // 2) % NZ, p % 2

    def dev(df=0, dz=0, dq=0, da=0):
        return ((f + df) % NFD, ((a + da) % 2) * 16 + ((z + dz + NZ) % NZ) * 2 + (q + dq) % 2)

    def row(a_, z_):
        return pl.multiple_of((a_ * NZ + z_) * 112, 16)

    peers = [dev(dz=1), dev(dz=-1), dev(dz=2), dev(dz=-2), dev(da=1)]
    freq_peers = [(df, dq) for df in (5, 3, 7, 1, 4, 2, 6, 0) for dq in range(2) if df or dq]

    own_r = pltpu.make_async_copy(resp.at[pl.ds(q * 8, 8)], rs.at[:, q], r_sem.at[0])
    own_r.start()

    barrier = pltpu.get_barrier_semaphore()
    for peer in peers + [dev(df=df, dq=dq) for df, dq in freq_peers]:
        pl.semaphore_signal(barrier, inc=1, device_id=peer, device_id_type=MESH)
    other_r = pltpu.make_async_remote_copy(
        src_ref=resp.at[pl.ds((1 - q) * 8, 8)], dst_ref=rs.at[:, q],
        send_sem=r_sem.at[1], recv_sem=r_sem.at[2], device_id=dev(dq=1), device_id_type=MESH)

    def spread(src_slot, dst, dst_slot, sends, recvs, ch):
        return [
            pltpu.make_async_remote_copy(
                src_ref=src_slot((f + df) % NFD, (q + dq) % 2), dst_ref=dst_slot(dst),
                send_sem=sends.at[ch, 2 * df + dq], recv_sem=recvs.at[ch, 2 * df + dq],
                device_id=dev(df=df, dq=dq), device_id_type=MESH)
            for df, dq in freq_peers]

    def sf_slot(ch):
        return lambda fd, qd: sf.at[ch, pl.ds(pl.multiple_of((fd * 2 + qd) * 16, 16), 16)]

    def sb_slot(ch):
        return lambda fd, qd: sb.at[ch, qd, pl.ds(pl.multiple_of(fd * 16, 16), 16)]

    def forward_copies(ch):
        return spread(sf_slot(ch), rf, lambda d: d.at[ch, q, pl.ds(pl.multiple_of(f * 16, 16), 16)], af_s, af_r, ch)

    def back_copies(ch):
        return spread(sb_slot(ch), rb, lambda d: d.at[ch, pl.ds(pl.multiple_of((f * 2 + q) * 16, 16), 16)],
                      ab_s, ab_r, ch)

    @scoped
    def analyse(ch, field, ready=None):
        sf[ch] = jnp.dot(fwd[...], field.astype(BF16), preferred_element_type=F32).astype(BF16)
        if ready is not None:
            ready()
        for copy in forward_copies(ch):
            copy.start()
        rf[ch, q, pl.ds(pl.multiple_of(f * 16, 16), 16)] = sf[ch, pl.ds(pl.multiple_of((f * 2 + q) * 16, 16), 16)]

    @scoped
    def collect(ch, par):
        for copy in forward_copies(ch):
            copy.wait_recv()
        for copy in forward_copies(ch):
            copy.wait_send()
        halves = []
        for core in range(2):
            parts = []
            for pair in range(V // 2):
                block = rf[ch, core, :, pair * 128:(pair + 1) * 128].astype(F32).T
                parts += [block[0:ROWS], block[ROWS:2 * ROWS]]
            halves.append(exchange(parts))
        for kp in range(V):
            x[par, ch, kp, pl.ds(row(a, z), 112), :] = jnp.concatenate(
                [halves[0][kp], halves[1][kp]], axis=0).astype(BF16)

    def message(ch, par, index, arriving=False):
        kp, d0, l0, d1, l1 = SENDS[index]
        dz, da = (d1 - d0 + 3) % NZ - 3, l1 - l0
        d, l = (d1, l1) if arriving else (d0, l0)
        ref = x.at[par, ch, kp, pl.ds(row((a + l) % 2, (z - d + NZ) % NZ), 112)]
        return pltpu.make_async_remote_copy(
            src_ref=ref, dst_ref=ref, send_sem=m_s.at[ch, index], recv_sem=m_r.at[par, ch, index],
            device_id=dev(dz=dz, da=da), device_id_type=MESH)

    def send_from(ch, par, kp, d, l):
        for index, (group, d0, l0, _, _) in enumerate(SENDS):
            if (d0, l0) == (d, l) and kp in (None, group):
                message(ch, par, index).start()

    @scoped
    def ring_start(ch, par):
        send_from(ch, par, None, 0, 0)

    def relay(ch, par, kp, d, l):
        index = [s[0:1] + s[3:5] for s in SENDS].index((kp, d, l))
        message(ch, par, index, arriving=True).wait_recv()
        send_from(ch, par, kp, d, l)

    @scoped
    def ring_drain(ch, par):
        for index in range(len(SENDS)):
            message(ch, par, index).wait_send()

    @scoped
    def apply(ch, par, n):
        sign = jnp.where(n % 2 == 0, 1.0, -1.0).astype(F32)
        shape = (ROWS, 128)
        low = lane_bit(shape, G)
        lanes = lax.broadcasted_iota(jnp.int32, shape, 1)
        groups = [[], []]
        last = {kp: place for place, (kp, _, _) in enumerate(ARRIVALS)}
        done = 0
        for kp in sorted(range(V), key=last.get):
            with jax.named_scope("gather%d" % kp):
                for each in ARRIVALS[done:last[kp] + 1]:
                    relay(ch, par, *each)
                done = last[kp] + 1
            if not groups[0]:
                @pl.when(n == 0)
                def _():
                    own_r.wait()
                    other_r.wait()
            for part in range(2):
                first = kp * G + part * (G // 2)
                prod[pl.ds(part * G * 112, G * 112), :] = jnp.dot(
                    rs[first:first + G // 2].reshape(G * 112, NS), x[par, ch, kp], preferred_element_type=F32)
            for core in range(2):
                re = im = None
                for kg in range(G):
                    base = kg * 224 + core * 112
                    re_k, im_k = prod[base:base + ROWS, :], prod[base + ROWS:base + 2 * ROWS, :]
                    mine = lanes % G == kg
                    re = re_k if re is None else jnp.where(mine, re_k, re)
                    im = im_k if im is None else jnp.where(mine, im_k, im)
                turned = jnp.where(low, -pltpu.roll(im, 128 - G, 1), pltpu.roll(im, G, 1))
                groups[core].append((kp, re + sign * turned))
        for core in range(2):
            parts = exchange([group for _, group in sorted(groups[core], key=lambda g: g[0])])
            for pair in range(V // 2):
                block = jnp.concatenate(
                    [parts[2 * pair], parts[2 * pair + 1], jnp.zeros((16, 128), F32)], axis=0)
                sb[ch, core, :, pair * 128:(pair + 1) * 128] = block.T.astype(BF16)
        for copy in back_copies(ch):
            copy.start()
        rb[ch, pl.ds(pl.multiple_of((f * 2 + q) * 16, 16), 16)] = sb[ch, q, pl.ds(pl.multiple_of(f * 16, 16), 16)]

    @scoped
    def synthesise(ch, n):
        for copy in back_copies(ch):
            copy.wait_recv()
        for copy in back_copies(ch):
            copy.wait_send()
        t = lax.broadcasted_iota(jnp.int32, (NT, LC), 0)
        inside = jnp.minimum(t, NT - t).astype(F32) < limits[0:1, ch * LC:(ch + 1) * LC]
        field = jnp.where(inside, jnp.dot(inv[...], rb[ch], preferred_element_type=F32), 0.0)
        fb[n % 2, ch] = field
        return field

    lanes8 = lax.broadcasted_iota(jnp.int32, (8, 128), 1)
    turned = jnp.concatenate([onset[...].astype(F32), jnp.zeros((NVD, 128 - ROWS), F32)], axis=1)
    for pair in range(2):
        first, second = (jnp.broadcast_to(turned[2 * pair + i:2 * pair + i + 1], (8, 128)) for i in range(2))
        limits[:, pair * 128:(pair + 1) * 128] = jnp.where(lanes8 < ROWS, first, pltpu.roll(second, ROWS, 1))
    for ch in range(CHUNKS):
        for pair in range(V // 2):
            first = ch * V + 2 * pair
            block = jnp.concatenate(
                [direct[:, first, :], direct[:, first + 1, :],
                 jnp.zeros((16, NT), F32)], axis=0)
            dt[ch, :, pair * 128:(pair + 1) * 128] = block.T
        analyse(ch, dt[ch], None if ch else lambda: pl.semaphore_wait(barrier, len(peers) + len(freq_peers)))
    collect(0, 0)
    ring_start(0, 0)
    other_r.start()

    def step(n, carry):
        par = n % 2
        apply(0, par, n)
        ring_drain(0, par)
        field = synthesise(0, n)

        @pl.when(n < 2 * ITERS - 1)
        def _():
            analyse(0, jnp.where(n % 2 == 0, field, field + dt[0]))
            collect(0, 1 - par)
            ring_start(0, 1 - par)
        return carry

    lax.fori_loop(0, 2 * ITERS, step, 0)

    for part, out in ((0, up_out), (1, coda_out)):
        for ch in range(CHUNKS):
            for pair in range(V // 2):
                block = fb[part, ch, :, pair * 128:(pair + 1) * 128].T
                for half in range(2):
                    v = ch * V + 2 * pair + half
                    out[:, v, :] = block[half * ROWS:(half + 1) * ROWS]


def body(response, direct, onset):
    fwd, inv = tables()
    vmem = pl.BlockSpec(memory_space=pltpu.VMEM)
    dma = pltpu.SemaphoreType.DMA
    return pl.pallas_call(
        kernel,
        name="marchenko",
        out_shape=[jax.ShapeDtypeStruct((ROWS, NVD, NT), F32)] * 2,
        in_specs=[pl.BlockSpec(memory_space=pl.ANY), vmem, vmem, vmem, vmem],
        out_specs=[vmem, vmem],
        scratch_shapes=[
            pltpu.VMEM((8, 2, 112, NS), BF16),
            pltpu.VMEM((2, CHUNKS, V, NS, 128), BF16),
            pltpu.VMEM((CHUNKS, 256, LC), BF16),
            pltpu.VMEM((CHUNKS, 2, 128, LC), BF16),
            pltpu.VMEM((CHUNKS, 2, 128, LC), BF16),
            pltpu.VMEM((CHUNKS, 256, LC), BF16),
            pltpu.VMEM((CHUNKS, NT, LC), F32),
            pltpu.VMEM((2, CHUNKS, NT, LC), F32),
            pltpu.VMEM((G * 224, 128), F32),
            pltpu.VMEM((8, 256), F32),
            dma((3,)),
            dma((CHUNKS, 16)), dma((CHUNKS, 16)), dma((CHUNKS, 16)), dma((CHUNKS, 16)),
            dma((CHUNKS, len(SENDS))), dma((2, CHUNKS, len(SENDS))),
        ],
        compiler_params=pltpu.CompilerParams(
            collective_id=0, has_side_effects=True, vmem_limit_bytes=60 * 2**20),
    )(response.reshape(16, 112, NS), direct, onset.T, fwd, inv)


def solution(mesh):
    placed = (P("freq", None, "rec", None), P("rec", "freq", None), P("rec", "freq"))
    return jax.shard_map(
        body, mesh=mesh, in_specs=placed,
        out_specs=(P("rec", "freq", None), P("rec", "freq", None)), check_vma=False)
```

```python
import math

import jax
import jax.numpy as jnp
import numpy as np
from jax import lax
from jax.experimental import pallas as pl
from jax.experimental.pallas import tpu as pltpu
from jax.sharding import PartitionSpec as P

NF, NT, ITERS = 128, 256, 2
NS, ROWS, NVD, NFD = 1792, 56, 4, 8
NZ = 8
CHUNKS = 1
V = NVD // CHUNKS
G = 8 // V
LC = 64 * V
MESH = pl.DeviceIdType.MESH
F32, BF16 = jnp.float32, jnp.bfloat16
EARLY = [1, 3]
SENDS = [
    (3, 0, 0, 1, 0), (2, 0, 0, 1, 0), (0, 0, 0, -1, 0), (0, 0, 0, 1, 0), (0, 0, 0, 0, 1), (1, 0, 0, 0, 1),
    (2, 0, 0, -1, 0), (3, 0, 0, -2, 0), (1, 0, 0, 1, 0), (1, 0, 0, -2, 0), (2, 0, 0, 0, 1), (0, 0, 0, 2, 0),
    (3, 0, 0, 0, 1), (0, -1, 0, -1, 1), (0, -1, 0, -2, 0), (0, 2, 0, 3, 0), (0, 2, 0, 2, 1), (0, -3, 1, 4, 1),
    (0, -3, 1, -3, 0), (0, 3, 0, 4, 0), (0, 3, 0, 3, 1), (0, 1, 0, 1, 1), (0, -1, 1, -3, 1), (0, -1, 1, -2, 1),
    (1, 1, 0, 2, 0), (1, 1, 0, 1, 1), (1, -2, 0, -1, 0), (1, -2, 0, -3, 0), (1, -2, 0, -2, 1), (1, -1, 0, -1, 1),
    (1, 2, 0, 3, 0), (1, -3, 0, 4, 0), (1, -3, 0, -3, 1), (1, 0, 1, 2, 1), (1, 2, 1, 4, 1), (1, 2, 1, 3, 1),
    (2, 1, 0, 2, 0), (2, -1, 0, -3, 0), (2, -1, 0, -2, 0), (2, -1, 0, -1, 1), (2, 4, 0, 3, 0), (2, 4, 0, 4, 1),
    (2, -3, 0, 4, 0), (2, -3, 0, -3, 1), (2, 2, 1, 1, 1), (2, 2, 1, 3, 1), (2, 2, 0, 2, 1), (2, -2, 0, -2, 1),
    (3, -2, 0, 4, 0), (3, -2, 0, -1, 0), (3, -2, 0, -2, 1), (3, -2, 0, -3, 0), (3, 1, 0, 2, 0), (3, 2, 0, 2, 1),
    (3, 2, 0, 3, 0), (3, 2, 1, 1, 1), (3, 2, 1, 3, 1), (3, -1, 0, -1, 1), (3, -2, 1, -3, 1), (3, 4, 0, 4, 1),
]
ARRIVALS = [
    (3, 1, 0), (0, -1, 0), (0, 0, 1), (2, 1, 0), (2, -1, 0), (1, 0, 1), (0, 1, 0), (2, 0, 1),
    (1, 1, 0), (3, 0, 1), (3, -2, 0), (1, -2, 0), (0, 2, 0), (3, 2, 0), (0, -2, 0), (0, -1, 1),
    (2, 2, 0), (2, -1, 1), (0, 1, 1), (2, -2, 0), (2, -3, 0), (1, 1, 1), (1, 2, 0), (1, 2, 1),
    (3, -2, 1), (3, -1, 0), (1, -2, 1), (1, -1, 0), (3, -3, 0), (0, 2, 1), (3, 4, 0), (0, 3, 0),
    (1, -3, 0), (3, 2, 1), (3, 3, 0), (2, 2, 1), (2, -2, 1), (1, 3, 0), (0, -2, 1), (2, -3, 1),
    (0, -3, 1), (2, 4, 0), (3, -1, 1), (3, -3, 1), (1, -1, 1), (1, 3, 1), (1, 4, 1), (3, 4, 1),
    (1, 4, 0), (0, 4, 0), (0, 3, 1), (3, 1, 1), (3, 3, 1), (1, -3, 1), (2, 1, 1), (2, 3, 1),
    (0, 4, 1), (0, -3, 0), (2, 3, 0), (2, 4, 1),
]

def tables():
    rho = np.arange(256)
    kg = rho % G
    part = (rho // G) % 2
    kp = (rho // (2 * G)) % V
    band = rho // 16
    bins = band * 8 + kp * G + kg + 1
    phase = ((np.arange(NT)[None, :] * bins[:, None]) % NT).astype(np.float64) * (2.0 * math.pi / NT)
    table = np.where(part[:, None] == 0, np.cos(phase), -np.sin(phase)).astype(np.float32)
    return jnp.asarray(table, dtype=BF16), jnp.asarray((table * (2.0 / NT)).T, dtype=BF16)


def scoped(function):
    def wrapped(*args):
        with jax.named_scope(function.__name__):
            return function(*args)
    return wrapped


def lane_bit(shape, stride):
    lanes = lax.broadcasted_iota(jnp.int32, shape, len(shape) - 1)
    return (lanes // stride) % 2 == 0


def exchange(arrays):
    shape = arrays[0].shape
    stride, span = 2 * G, 1
    while span < V:
        low = lane_bit(shape, stride)
        out = list(arrays)
        for i in range(V):
            if (i // span) % 2 == 0:
                first, second = arrays[i], arrays[i + span]
                out[i] = jnp.where(low, first, pltpu.roll(second, stride, 1))
                out[i + span] = jnp.where(low, pltpu.roll(first, 128 - stride, 1), second)
        arrays = out
        stride, span = stride * 2, span * 2
    return arrays


def kernel(
    resp, direct_in, onset_in, fwd_in, inv_in, fields,
    direct, onset, fwd, inv, fb, rs, x, sf, rf, sb, rb, dt, prod, limits, in_sem, out_sem,
    r_sem, af_s, af_r, ab_s, ab_r, m_s, m_r,
):
    f = lax.axis_index("freq")
    p = lax.axis_index("rec")
    a, z, q = p // 16, (p // 2) % NZ, p % 2

    def dev(df=0, dz=0, dq=0, da=0):
        return ((f + df) % NFD, ((a + da) % 2) * 16 + ((z + dz + NZ) % NZ) * 2 + (q + dq) % 2)

    def row(a_, z_):
        return pl.multiple_of((a_ * NZ + z_) * 112, 16)

    peers = [dev(dz=1), dev(dz=-1), dev(dz=2), dev(dz=-2), dev(da=1)]
    freq_peers = [(df, dq) for df in (5, 3, 7, 1, 4, 2, 6, 0) for dq in range(2) if df or dq]

    barrier = pltpu.get_barrier_semaphore()
    for peer in peers + [dev(df=df, dq=dq) for df, dq in freq_peers]:
        pl.semaphore_signal(barrier, inc=1, device_id=peer, device_id_type=MESH)
    other_r = pltpu.make_async_remote_copy(
        src_ref=resp.at[pl.ds((1 - q) * 8, 8)], dst_ref=rs.at[:, q],
        send_sem=r_sem.at[1], recv_sem=r_sem.at[2], device_id=dev(dq=1), device_id_type=MESH)

    inputs = [
        pltpu.make_async_copy(source, held, in_sem.at[place]) for place, (source, held) in enumerate(
            ((onset_in, onset), (direct_in, direct), (fwd_in, fwd), (inv_in, inv)))]
    for copy in inputs:
        copy.start()
    own_r = pltpu.make_async_copy(resp.at[pl.ds(q * 8, 8)], rs.at[:, q], r_sem.at[0])
    own_r.start()
    for copy in inputs:
        copy.wait()

    def result(part):
        return pltpu.make_async_copy(fb.at[part], fields.at[part], out_sem.at[part])

    def spread(src_slot, dst, dst_slot, sends, recvs, ch):
        return [
            pltpu.make_async_remote_copy(
                src_ref=src_slot((f + df) % NFD, (q + dq) % 2), dst_ref=dst_slot(dst),
                send_sem=sends.at[ch, 2 * df + dq], recv_sem=recvs.at[ch, 2 * df + dq],
                device_id=dev(df=df, dq=dq), device_id_type=MESH)
            for df, dq in freq_peers]

    def sf_slot(ch):
        return lambda fd, qd: sf.at[ch, pl.ds(pl.multiple_of((fd * 2 + qd) * 16, 16), 16)]

    def sb_slot(ch):
        return lambda fd, qd: sb.at[ch, qd, pl.ds(pl.multiple_of(fd * 16, 16), 16)]

    def forward_copies(ch):
        return spread(sf_slot(ch), rf, lambda d: d.at[ch, q, pl.ds(pl.multiple_of(f * 16, 16), 16)], af_s, af_r, ch)

    def back_copies(ch):
        return spread(sb_slot(ch), rb, lambda d: d.at[ch, pl.ds(pl.multiple_of((f * 2 + q) * 16, 16), 16)],
                      ab_s, ab_r, ch)

    @scoped
    def analyse(ch, field, ready=None):
        sf[ch] = jnp.dot(fwd[...], field.astype(BF16), preferred_element_type=F32).astype(BF16)
        if ready is not None:
            ready()
        for copy in forward_copies(ch):
            copy.start()
        rf[ch, q, pl.ds(pl.multiple_of(f * 16, 16), 16)] = sf[ch, pl.ds(pl.multiple_of((f * 2 + q) * 16, 16), 16)]

    @scoped
    def collect(ch, par):
        for copy in forward_copies(ch):
            copy.wait_recv()
        for copy in forward_copies(ch):
            copy.wait_send()
        halves = []
        for core in range(2):
            parts = []
            for pair in range(V // 2):
                block = rf[ch, core, :, pair * 128:(pair + 1) * 128].astype(F32).T
                parts += [block[0:ROWS], block[ROWS:2 * ROWS]]
            halves.append(exchange(parts))
        for kp in range(V):
            x[par, ch, kp, pl.ds(row(a, z), 112), :] = jnp.concatenate(
                [halves[0][kp], halves[1][kp]], axis=0).astype(BF16)

    def message(ch, par, index, arriving=False):
        kp, d0, l0, d1, l1 = SENDS[index]
        dz, da = (d1 - d0 + 3) % NZ - 3, l1 - l0
        d, l = (d1, l1) if arriving else (d0, l0)
        ref = x.at[par, ch, kp, pl.ds(row((a + l) % 2, (z - d + NZ) % NZ), 112)]
        return pltpu.make_async_remote_copy(
            src_ref=ref, dst_ref=ref, send_sem=m_s.at[ch, index], recv_sem=m_r.at[par, ch, index],
            device_id=dev(dz=dz, da=da), device_id_type=MESH)

    def send_from(ch, par, kp, d, l):
        for index, (group, d0, l0, _, _) in enumerate(SENDS):
            if (d0, l0) == (d, l) and kp in (None, group):
                message(ch, par, index).start()

    @scoped
    def ring_start(ch, par):
        send_from(ch, par, None, 0, 0)

    def relay(ch, par, kp, d, l):
        index = [s[0:1] + s[3:5] for s in SENDS].index((kp, d, l))
        message(ch, par, index, arriving=True).wait_recv()
        send_from(ch, par, kp, d, l)

    @scoped
    def ring_drain(ch, par):
        for index in range(len(SENDS)):
            message(ch, par, index).wait_send()

    @scoped
    def apply(ch, par, n):
        sign = jnp.where(n % 2 == 0, 1.0, -1.0).astype(F32)
        shape = (ROWS, 128)
        low = lane_bit(shape, G)
        lanes = lax.broadcasted_iota(jnp.int32, shape, 1)
        groups = [[], []]
        holders = {(kp, d, l) for kp, d, l, _, _ in SENDS}
        relays = [each for each in ARRIVALS if each in holders]
        leaves = [each for each in ARRIVALS if each not in holders]
        with jax.named_scope("gather"):
            for each in relays + [each for each in leaves if each[0] in EARLY]:
                relay(ch, par, *each)

        @pl.when(n == 0)
        def _():
            own_r.wait()
            other_r.wait()

        for kp in EARLY + [kp for kp in range(V) if kp not in EARLY]:
            if kp not in EARLY and len(groups[0]) == len(EARLY):
                with jax.named_scope("gather_late"):
                    for each in leaves:
                        if each[0] not in EARLY:
                            relay(ch, par, *each)
            prod[...] = jnp.dot(
                rs[kp * G:(kp + 1) * G].reshape(G * 224, NS), x[par, ch, kp], preferred_element_type=F32)
            for core in range(2):
                re = im = None
                for kg in range(G):
                    base = kg * 224 + core * 112
                    re_k, im_k = prod[base:base + ROWS, :], prod[base + ROWS:base + 2 * ROWS, :]
                    mine = lanes % G == kg
                    re = re_k if re is None else jnp.where(mine, re_k, re)
                    im = im_k if im is None else jnp.where(mine, im_k, im)
                turned = jnp.where(low, -pltpu.roll(im, 128 - G, 1), pltpu.roll(im, G, 1))
                groups[core].append((kp, re + sign * turned))
        for core in range(2):
            parts = exchange([group for _, group in sorted(groups[core], key=lambda g: g[0])])
            for pair in range(V // 2):
                block = jnp.concatenate(
                    [parts[2 * pair], parts[2 * pair + 1], jnp.zeros((16, 128), F32)], axis=0)
                sb[ch, core, :, pair * 128:(pair + 1) * 128] = block.T.astype(BF16)
        for copy in back_copies(ch):
            copy.start()
        rb[ch, pl.ds(pl.multiple_of((f * 2 + q) * 16, 16), 16)] = sb[ch, q, pl.ds(pl.multiple_of(f * 16, 16), 16)]

    @scoped
    def synthesise(ch, n):
        for copy in back_copies(ch):
            copy.wait_recv()
        for copy in back_copies(ch):
            copy.wait_send()
        t = lax.broadcasted_iota(jnp.int32, (NT, LC), 0)
        inside = jnp.minimum(t, NT - t).astype(F32) < limits[0:1, ch * LC:(ch + 1) * LC]
        field = jnp.where(inside, jnp.dot(inv[...], rb[ch], preferred_element_type=F32), 0.0)
        fb[n % 2, ch] = field
        return field

    lanes8 = lax.broadcasted_iota(jnp.int32, (8, 128), 1)
    turned = jnp.concatenate([onset[...].astype(F32), jnp.zeros((NVD, 128 - ROWS), F32)], axis=1)
    for pair in range(2):
        first, second = (jnp.broadcast_to(turned[2 * pair + i:2 * pair + i + 1], (8, 128)) for i in range(2))
        limits[:, pair * 128:(pair + 1) * 128] = jnp.where(lanes8 < ROWS, first, pltpu.roll(second, ROWS, 1))
    for ch in range(CHUNKS):
        for pair in range(V // 2):
            first = ch * V + 2 * pair
            block = jnp.concatenate(
                [direct[:, first, :], direct[:, first + 1, :],
                 jnp.zeros((16, NT), F32)], axis=0)
            dt[ch, :, pair * 128:(pair + 1) * 128] = block.T
        analyse(ch, dt[ch], None if ch else lambda: pl.semaphore_wait(barrier, len(peers) + len(freq_peers)))
    collect(0, 0)
    ring_start(0, 0)
    other_r.start()

    def step(n, carry):
        par = n % 2
        apply(0, par, n)
        ring_drain(0, par)
        field = synthesise(0, n)

        @pl.when(n < 2 * ITERS - 1)
        def _():
            @pl.when(n == 2 * ITERS - 2)
            def _():
                result(0).start()

            analyse(0, jnp.where(n % 2 == 0, field, field + dt[0]))
            collect(0, 1 - par)
            ring_start(0, 1 - par)
        return carry

    lax.fori_loop(0, 2 * ITERS, step, 0)
    result(1).start()
    result(0).wait()
    result(1).wait()


def turn(fields, up_out, coda_out):
    for part, out in ((0, up_out), (1, coda_out)):
        for ch in range(CHUNKS):
            for pair in range(V // 2):
                block = fields[part, ch, :, pair * 128:(pair + 1) * 128].T
                for half in range(2):
                    out[:, ch * V + 2 * pair + half, :] = block[half * ROWS:(half + 1) * ROWS]


def body(response, direct, onset):
    fwd, inv = tables()
    vmem, hbm = pl.BlockSpec(memory_space=pltpu.VMEM), pl.BlockSpec(memory_space=pltpu.HBM)
    dma = pltpu.SemaphoreType.DMA
    fields = pl.pallas_call(
        kernel,
        name="marchenko",
        out_shape=jax.ShapeDtypeStruct((2, CHUNKS, NT, LC), F32),
        in_specs=[hbm] * 5,
        out_specs=hbm,
        scratch_shapes=[
            pltpu.VMEM((ROWS, NVD, NT), F32),
            pltpu.VMEM((NVD, ROWS), jnp.int32),
            pltpu.VMEM((256, NT), BF16),
            pltpu.VMEM((NT, 256), BF16),
            pltpu.VMEM((2, CHUNKS, NT, LC), F32),
            pltpu.VMEM((8, 2, 112, NS), BF16),
            pltpu.VMEM((2, CHUNKS, V, NS, 128), BF16),
            pltpu.VMEM((CHUNKS, 256, LC), BF16),
            pltpu.VMEM((CHUNKS, 2, 128, LC), BF16),
            pltpu.VMEM((CHUNKS, 2, 128, LC), BF16),
            pltpu.VMEM((CHUNKS, 256, LC), BF16),
            pltpu.VMEM((CHUNKS, NT, LC), F32),
            pltpu.VMEM((G * 224, 128), F32),
            pltpu.VMEM((8, 256), F32),
            dma((4,)), dma((2,)),
            dma((3,)),
            dma((CHUNKS, 16)), dma((CHUNKS, 16)), dma((CHUNKS, 16)), dma((CHUNKS, 16)),
            dma((CHUNKS, len(SENDS))), dma((2, CHUNKS, len(SENDS))),
        ],
        compiler_params=pltpu.CompilerParams(
            collective_id=0, has_side_effects=True, vmem_limit_bytes=58 * 2**20),
    )(response.reshape(16, 112, NS), direct, onset.T, fwd, inv)
    return pl.pallas_call(
        turn,
        name="turn",
        out_shape=[jax.ShapeDtypeStruct((ROWS, NVD, NT), F32)] * 2,
        in_specs=[vmem],
        out_specs=[vmem, vmem],
        compiler_params=pltpu.CompilerParams(vmem_limit_bytes=8 * 2**20),
    )(fields)


def solution(mesh):
    placed = (P("freq", None, "rec", None), P("rec", "freq", None), P("rec", "freq"))
    return jax.shard_map(
        body, mesh=mesh, in_specs=placed,
        out_specs=(P("rec", "freq", None), P("rec", "freq", None)), check_vma=False)
```
